8 devices in a mesh: side: 2 (over z, y), rep: 4 (over x, core).
Axes of the slice: x: 2, y: 2, z: 1, core: 2. Of those that a mesh axis runs over, the one named last changes fastest.
Arguments:
- w_up: float32 [2, 1, 3072, 8192], P('side', None, 'rep')
- w_down: float32 [2, 1, 8192, 3072], P('side', None, None, 'rep')
- g_up: float32 [2, 1, 3072, 8192], P('side', None, 'rep')
- g_down: float32 [2, 1, 8192, 3072], P('side', None, None, 'rep')
- learn_rate: float32 [], replicated
- prompts: bfloat16 [2, 8192, 3072], P('side', 'rep')
- prompt_lens: int32 [4], P('rep')
Outputs:
- output 1: float32 [2, 1, 3072, 8192], P('side', None, 'rep')
- output 2: float32 [2, 1, 8192, 3072], P('side', None, None, 'rep')
- output 3: bfloat16 [2, 8192, 3072], P('side', 'rep')
All inputs are finite; a program needn't handle non-finite values.
Results may differ from the reference program's by a relative error of at most 0.001.
Values are sent between devices in bfloat16 or wider.
A program may use at most 1 GiB of HBM per device.

```python
import jax
import jax.numpy as jnp
from jax import lax

SIDE_DEVS = 2
REP_DEVS = 4
MODEL_DIM = 3072
FFN_DIM = 8192
LAYERS = 1
TOKENS = 2048
TP_WAYS = SIDE_DEVS // 2
FF_PIECE = FFN_DIM // TP_WAYS
D_PIECE = MODEL_DIM // TP_WAYS


def draw_lens(len_key):
    key_a, key_b = jax.random.split(len_key)
    low_len = max(1, TOKENS // 32)
    base_lens = jax.random.randint(key_a, (REP_DEVS,), low_len, TOKENS + 1, jnp.int32)
    full_slot = jax.random.randint(key_b, (), 0, REP_DEVS, jnp.int32)
    return jnp.where(jnp.arange(REP_DEVS) == full_slot, TOKENS, base_lens).astype(jnp.int32)


def setup_inputs(seed: int = 0) -> dict:
    sub_keys = jax.random.split(jax.random.key(seed), 7)
    up_shape = (TP_WAYS, LAYERS, MODEL_DIM, FF_PIECE)
    down_shape = (TP_WAYS, LAYERS, FF_PIECE, MODEL_DIM)
    up_scale = MODEL_DIM ** -0.5
    down_scale = 0.7 * FFN_DIM ** -0.5
    w_up = jax.random.normal(sub_keys[0], up_shape, jnp.float32) * up_scale
    w_down = jax.random.normal(sub_keys[1], down_shape, jnp.float32) * down_scale
    g_up = jax.random.normal(sub_keys[2], up_shape, jnp.float32) * up_scale
    g_down = jax.random.normal(sub_keys[3], down_shape, jnp.float32) * down_scale
    learn_rate = jax.random.uniform(sub_keys[4], (), jnp.float32, 0.02, 0.25)
    gen_rows = jax.random.normal(sub_keys[5], (TP_WAYS, REP_DEVS * TOKENS, D_PIECE), jnp.float32)
    prompts = jnp.concatenate([jnp.zeros_like(gen_rows), gen_rows], axis=0).astype(jnp.bfloat16)
    return {
        "w_up": jnp.concatenate([w_up, jnp.zeros_like(w_up)], axis=0),
        "w_down": jnp.concatenate([w_down, jnp.zeros_like(w_down)], axis=0),
        "g_up": jnp.concatenate([g_up, jnp.zeros_like(g_up)], axis=0),
        "g_down": jnp.concatenate([g_down, jnp.zeros_like(g_down)], axis=0),
        "learn_rate": learn_rate,
        "prompts": prompts,
        "prompt_lens": draw_lens(sub_keys[6]),
    }


def reference(w_up, w_down, g_up, g_down, learn_rate, prompts, prompt_lens):
    new_up = w_up - learn_rate * g_up
    new_down = w_down - learn_rate * g_down
    up_bf = new_up[:TP_WAYS].astype(jnp.bfloat16)
    down_bf = new_down[:TP_WAYS].astype(jnp.bfloat16)
    up_full = jnp.transpose(up_bf, (1, 2, 0, 3)).reshape(LAYERS, MODEL_DIM, FFN_DIM)
    down_full = jnp.transpose(down_bf, (1, 0, 2, 3)).reshape(LAYERS, FFN_DIM, MODEL_DIM)
    x_full = jnp.transpose(prompts[TP_WAYS:], (1, 0, 2)).reshape(REP_DEVS, TOKENS, MODEL_DIM)

    def layer_step(h_rows, layer_w):
        up_layer, down_layer = layer_w
        pre_act = jnp.dot(h_rows, up_layer, preferred_element_type=jnp.float32)
        act_bf = jax.nn.gelu(pre_act, approximate=True).astype(jnp.bfloat16)
        part_sum = jnp.dot(act_bf, down_layer, preferred_element_type=jnp.float32)
        return (h_rows.astype(jnp.float32) + part_sum).astype(jnp.bfloat16), None

    def one_replica(replica_in):
        row_block, length = replica_in
        h_rows, _ = lax.scan(layer_step, row_block, (up_full, down_full))
        keep_mask = jnp.arange(TOKENS)[:, None] < length
        return jnp.where(keep_mask, h_rows, jnp.zeros_like(h_rows))

    y_full = lax.map(one_replica, (x_full, prompt_lens))
    y_gen = jnp.transpose(y_full.reshape(REP_DEVS * TOKENS, TP_WAYS, D_PIECE), (1, 0, 2))
    outputs = jnp.concatenate([jnp.zeros_like(y_gen), y_gen], axis=0)
    return new_up, new_down, outputs
```

```python
import functools

import jax
import jax.numpy as jnp
from jax import lax
from jax.experimental import pallas as pl
from jax.experimental.pallas import tpu as pltpu
from jax.sharding import PartitionSpec as P

MESH = pl.DeviceIdType.MESH
CHUNK = 256
HEAD = 3
ROWS = 512
COLS = 768
OUT_ROWS = 256


def stream_kernel(
    up_ref, down_ref, up_head, down_head, x_hbm,
    y_hbm, up_all, down_all,
    x_ref, total, up_slot, down_slot, up_bounce, down_bounce, y_stage,
    send_y, recv_y, send_x, recv_x, send_d, recv_d, send_f, recv_f,
    load_sem, head_sem, x_sem, y_sem,
):
    side = lax.axis_index("side")
    me = lax.axis_index("rep")
    mate = me + 1 - 2 * lax.rem(me, 2)
    across = lax.rem(me + 2, 4)
    width = up_ref.shape[0]
    count = up_ref.shape[1] // CHUNK
    tokens = x_ref.shape[0]

    barrier = pltpu.get_barrier_semaphore()
    for peer in ((side, mate), (side, across), (1 - side, me)):
        pl.semaphore_signal(barrier, inc=1, device_id=peer, device_id_type=MESH)
    pl.semaphore_wait(barrier, 3)

    def wide(c):
        return pl.ds(pl.multiple_of(c * CHUNK, CHUNK), CHUNK)

    def piece(q):
        return pl.ds(pl.multiple_of(q * width, width), width)

    def remote(src, dst, send, recv, peer):
        return pltpu.make_async_remote_copy(
            src_ref=src, dst_ref=dst, send_sem=send, recv_sem=recv, device_id=peer, device_id_type=MESH
        )

    def down_link(c):
        return (
            remote(up_ref.at[:, wide(c)], up_all.at[c, piece(me), :], send_y.at[0, c], recv_y.at[0, c], (1, me)),
            remote(down_ref.at[wide(c), :], down_all.at[c, :, piece(me)], send_y.at[1, c], recv_y.at[1, c], (1, me)),
        )

    def relay(c, q, send, recv, peer):
        up_part = up_all.at[c, piece(q), :]
        down_part = down_all.at[c, :, piece(q)]
        return (
            remote(up_part, up_part, send.at[0, c], recv.at[0, c], (1, peer)),
            remote(down_part, down_part, send.at[1, c], recv.at[1, c], (1, peer)),
        )

    def to_across(c):
        return relay(c, me, send_x, recv_x, across)

    def to_mate(c):
        return relay(c, me, send_d, recv_d, mate)

    def forward(c):
        return relay(c, across, send_f, recv_f, mate)

    def loads(c):
        slot = lax.rem(c, 2)
        return (
            pltpu.make_async_copy(up_all.at[c], up_slot.at[slot], load_sem.at[0, slot]),
            pltpu.make_async_copy(down_all.at[c], down_slot.at[slot], load_sem.at[1, slot]),
        )

    @pl.when(side == 0)
    def _():
        def send(c, carry):
            for copy in down_link(c):
                copy.start()

            @pl.when(c >= HEAD + 2)
            def _():
                for copy in down_link(c - 2):
                    copy.wait_send()

            return carry

        lax.fori_loop(HEAD, count, send, 0)
        for c in (count - 2, count - 1):
            for copy in down_link(c):
                copy.wait_send()

    @pl.when(side == 1)
    def _():
        x_copy = pltpu.make_async_copy(x_hbm, x_ref, x_sem)
        heads = (
            pltpu.make_async_copy(up_head, up_bounce, head_sem.at[0]),
            pltpu.make_async_copy(down_head, down_bounce, head_sem.at[1]),
        )
        for copy in heads:
            copy.start()
        for copy in heads:
            copy.wait()
        x_copy.start()
        places = []
        for c in range(HEAD):
            part = slice(c * CHUNK, (c + 1) * CHUNK)
            places.append(
                pltpu.make_async_copy(up_bounce.at[:, part], up_all.at[c, piece(me), :], send_y.at[0, c])
            )
            places.append(
                pltpu.make_async_copy(down_bounce.at[part, :], down_all.at[c, :, piece(me)], send_y.at[1, c])
            )
        for copy in places:
            copy.start()
        for copy in places:
            copy.wait()
        total[...] = jnp.zeros_like(total)
        x_copy.wait()

        def compute(slot):
            def block(t, carry):
                rows = pl.ds(pl.multiple_of(t * ROWS, ROWS), ROWS)
                pre = jnp.dot(x_ref[rows, :], up_slot[slot], preferred_element_type=jnp.float32)
                act = jax.nn.gelu(pre, approximate=True).astype(jnp.bfloat16)
                for n in range(0, total.shape[1], COLS):
                    total[rows, n : n + COLS] += jnp.dot(
                        act, down_slot[slot, :, n : n + COLS], preferred_element_type=jnp.float32
                    )
                return carry

            lax.fori_loop(0, tokens // ROWS, block, 0)

        def turn(c, carry):
            @pl.when(c < count)
            def _():
                @pl.when(c >= HEAD)
                def _():
                    for copy in down_link(c):
                        copy.wait_recv()

                for copy in to_across(c) + to_mate(c):
                    copy.start()

            @pl.when(c >= 2)
            def _():
                for copy in loads(c - 2):
                    copy.wait()
                compute(lax.rem(c, 2))

            @pl.when((c >= 1) & (c <= count))
            def _():
                for copy in to_across(c - 1):
                    copy.wait_recv()
                for copy in forward(c - 1):
                    copy.start()
                for copy in to_mate(c - 1) + forward(c - 1):
                    copy.wait_recv()
                for copy in loads(c - 1):
                    copy.start()

            return carry

        lax.fori_loop(0, count + 2, turn, 0)

        def drain(c, carry):
            for copy in to_across(c) + to_mate(c) + forward(c):
                copy.wait_send()
            return carry

        lax.fori_loop(0, count, drain, 0)

        def out_copy(t):
            rows = pl.ds(pl.multiple_of(t * OUT_ROWS, OUT_ROWS), OUT_ROWS)
            slot = lax.rem(t, 2)
            return pltpu.make_async_copy(y_stage.at[slot], y_hbm.at[rows, :], y_sem.at[slot])

        def finish(t, carry):
            @pl.when(t >= 2)
            def _():
                out_copy(t - 2).wait()

            rows = pl.ds(pl.multiple_of(t * OUT_ROWS, OUT_ROWS), OUT_ROWS)
            y_stage[lax.rem(t, 2)] = (x_ref[rows, :].astype(jnp.float32) + total[rows, :]).astype(jnp.bfloat16)
            out_copy(t).start()
            return carry

        steps = tokens // OUT_ROWS
        lax.fori_loop(0, steps, finish, 0)
        for t in (steps - 2, steps - 1):
            out_copy(t).wait()


def stream_mlp(up_bf, down_bf, up_head, down_head, x):
    width, hidden = up_bf.shape
    tokens, model = x.shape
    count = hidden // CHUNK
    sems = pltpu.SemaphoreType.DMA((2, count))
    anywhere = pl.BlockSpec(memory_space=pl.ANY)
    bf16 = jnp.bfloat16
    return pl.pallas_call(
        stream_kernel,
        out_shape=(
            jax.ShapeDtypeStruct((tokens, model), bf16),
            jax.ShapeDtypeStruct((count, model, CHUNK), bf16),
            jax.ShapeDtypeStruct((count, CHUNK, model), bf16),
        ),
        in_specs=[anywhere] * 5,
        out_specs=(anywhere,) * 3,
        scratch_shapes=[
            pltpu.VMEM((tokens, model), bf16),
            pltpu.VMEM((tokens, model), jnp.float32),
            pltpu.VMEM((2, model, CHUNK), bf16),
            pltpu.VMEM((2, CHUNK, model), bf16),
            pltpu.VMEM((width, HEAD * CHUNK), bf16),
            pltpu.VMEM((HEAD * CHUNK, width), bf16),
            pltpu.VMEM((2, OUT_ROWS, model), bf16),
        ]
        + [sems] * 8
        + [
            pltpu.SemaphoreType.DMA((2, 2)),
            pltpu.SemaphoreType.DMA((2,)),
            pltpu.SemaphoreType.DMA,
            pltpu.SemaphoreType.DMA((2,)),
        ],
        compiler_params=pltpu.CompilerParams(
            collective_id=0, has_side_effects=True, vmem_limit_bytes=63 * 1024 * 1024
        ),
        cost_estimate=pl.CostEstimate(
            flops=4 * tokens * model * hidden, bytes_accessed=8 * model * hidden, transcendentals=tokens * hidden
        ),
    )(up_bf, down_bf, up_head, down_head, x)


def solution(mesh):
    up_spec = P("side", None, "rep", None)
    down_spec = P("side", None, None, "rep")
    act_spec = P("side", "rep", None)
    cross = [(r, r + mesh.shape["rep"]) for r in range(mesh.shape["rep"])]
    head = HEAD * CHUNK

    def device_step(w_up, w_down, g_up, g_down, learn_rate, prompts, prompt_lens):
        bf16 = jnp.bfloat16
        up_first = (w_up[0, 0, :, :head] - learn_rate * g_up[0, 0, :, :head]).astype(bf16)
        down_first = (w_down[0, 0, :head, :] - learn_rate * g_down[0, 0, :head, :]).astype(bf16)
        up_head = lax.ppermute(up_first, ("side", "rep"), cross)
        down_head = lax.ppermute(down_first, ("side", "rep"), cross)
        w_up, w_down, g_up, g_down, up_first, down_first = lax.optimization_barrier(
            (w_up, w_down, g_up, g_down, up_first, down_first)
        )
        new_up = w_up - learn_rate * g_up
        new_down = w_down - learn_rate * g_down
        y = stream_mlp(
            new_up[0, 0].astype(bf16), new_down[0, 0].astype(bf16), up_head, down_head, prompts[0]
        )[0]
        keep = (jnp.arange(y.shape[0])[:, None] < prompt_lens[0]) & (lax.axis_index("side") == 1)
        out = jnp.where(keep, y, jnp.zeros_like(y))
        return new_up, new_down, out[None]

    return jax.shard_map(
        device_step,
        mesh=mesh,
        in_specs=(up_spec, down_spec, up_spec, down_spec, P(), act_spec, P("rep")),
        out_specs=(up_spec, down_spec, act_spec),
        check_vma=False,
    )
```

```python
import jax
import jax.numpy as jnp
from jax import lax
from jax.experimental import pallas as pl
from jax.experimental.pallas import tpu as pltpu
from jax.sharding import PartitionSpec as P

MESH = pl.DeviceIdType.MESH
CHUNK = 256
HEAD = 1
ROWS = 512
COLS = 768
OUT_ROWS = 256
UP_TILE = 32
DOWN_TILE = 512
EARLY = 12
DEPTH = 3
STAGES = 4


def stream_kernel(
    up_w, up_g, down_w, down_g, rate_ref, up_head, down_head, x_hbm, order_ref,
    y_hbm, up_all, down_all,
    x_ref, total, up_slot, down_slot, up_bounce, down_bounce, y_stage,
    send_y, recv_y, send_x, recv_x, send_d, recv_d, send_f, recv_f,
    load_sem, fetch_sem, head_sem, x_sem, y_sem,
):
    side = lax.axis_index("side")
    me = lax.axis_index("rep")
    mate = me + 1 - 2 * lax.rem(me, 2)
    across = lax.rem(me + 2, 4)
    width = up_w.shape[0]
    count = up_w.shape[1] // CHUNK
    tokens = x_ref.shape[0]

    barrier = pltpu.get_barrier_semaphore()
    for peer in ((side, mate), (side, across), (1 - side, me)):
        pl.semaphore_signal(barrier, inc=1, device_id=peer, device_id_type=MESH)
    pl.semaphore_wait(barrier, 3)

    def wide(c):
        return pl.ds(pl.multiple_of(c * CHUNK, CHUNK), CHUNK)

    def piece(q):
        return pl.ds(pl.multiple_of(q * width, width), width)

    def remote(src, dst, send, recv, peer):
        return pltpu.make_async_remote_copy(
            src_ref=src, dst_ref=dst, send_sem=send, recv_sem=recv, device_id=peer, device_id_type=MESH
        )

    def down_link(c):
        stage = lax.rem(c, STAGES)
        up_part = up_slot.at[0, piece(stage), :]
        down_part = down_slot.at[0, :, piece(stage)]
        return (
            remote(up_part, up_all.at[c, piece(me), :], send_y.at[0, c], recv_y.at[0, c], (1, me)),
            remote(down_part, down_all.at[c, :, piece(me)], send_y.at[1, c], recv_y.at[1, c], (1, me)),
        )

    def relay(c, q, send, recv, peer):
        up_part = up_all.at[c, piece(q), :]
        down_part = down_all.at[c, :, piece(q)]
        return (
            remote(up_part, up_part, send.at[0, c], recv.at[0, c], (1, peer)),
            remote(down_part, down_part, send.at[1, c], recv.at[1, c], (1, peer)),
        )

    def to_across(c):
        return relay(c, me, send_x, recv_x, across)

    def to_mate(c):
        return relay(c, me, send_d, recv_d, mate)

    def forward(c):
        return relay(c, across, send_f, recv_f, mate)

    def loads(c):
        slot = lax.rem(c, 2)
        return (
            pltpu.make_async_copy(up_all.at[c], up_slot.at[slot], load_sem.at[0, slot]),
            pltpu.make_async_copy(down_all.at[c], down_slot.at[slot], load_sem.at[1, slot]),
        )

    @pl.when(side == 0)
    def _():
        rate = rate_ref[0]

        def up_view(slot, k):
            return total.at[pl.ds(0, width), pl.ds(pl.multiple_of((2 * slot + k) * CHUNK, CHUNK), CHUNK)]

        def down_view(slot, k):
            return total.at[pl.ds(pl.multiple_of(width + (2 * slot + k) * CHUNK, CHUNK), CHUNK), pl.ds(0, width)]

        def fetches(c):
            slot = lax.rem(c, 2)
            return (
                pltpu.make_async_copy(up_w.at[:, wide(c)], up_view(slot, 0), fetch_sem.at[slot, 0]),
                pltpu.make_async_copy(up_g.at[:, wide(c)], up_view(slot, 1), fetch_sem.at[slot, 1]),
                pltpu.make_async_copy(down_w.at[wide(c), :], down_view(slot, 0), fetch_sem.at[slot, 2]),
                pltpu.make_async_copy(down_g.at[wide(c), :], down_view(slot, 1), fetch_sem.at[slot, 3]),
            )

        for c in (HEAD, HEAD + 1):
            for copy in fetches(c):
                copy.start()

        def send(c, carry):
            @pl.when(c < count)
            def _():
                slot = lax.rem(c, 2)
                stage = lax.rem(c, STAGES)
                for copy in fetches(c):
                    copy.wait()

                @pl.when(c >= HEAD + STAGES)
                def _():
                    for copy in down_link(c - STAGES):
                        copy.wait_send()

                up_slot[0, piece(stage), :] = (up_view(slot, 0)[...] - rate * up_view(slot, 1)[...]).astype(jnp.bfloat16)
                down_slot[0, :, piece(stage)] = (
                    down_view(slot, 0)[...] - rate * down_view(slot, 1)[...]
                ).astype(jnp.bfloat16)

                @pl.when(c + 2 < count)
                def _():
                    for copy in fetches(c + 2):
                        copy.start()

            @pl.when(c > HEAD)
            def _():
                for copy in down_link(c - 1):
                    copy.start()

            return carry

        lax.fori_loop(HEAD, count + 1, send, 0)
        for c in range(count - STAGES, count):
            for copy in down_link(c):
                copy.wait_send()

    @pl.when(side == 1)
    def _():
        x_copy = pltpu.make_async_copy(x_hbm, x_ref, x_sem)
        heads = (
            pltpu.make_async_copy(up_head, up_bounce, head_sem.at[0]),
            pltpu.make_async_copy(down_head, down_bounce, head_sem.at[1]),
        )
        for copy in heads:
            copy.start()
        for copy in heads:
            copy.wait()
        x_copy.start()
        places = []
        for c in range(HEAD):
            part = slice(c * CHUNK, (c + 1) * CHUNK)
            places.append(
                pltpu.make_async_copy(up_bounce.at[:, part], up_all.at[c, piece(me), :], send_y.at[0, c])
            )
            places.append(
                pltpu.make_async_copy(down_bounce.at[part, :], down_all.at[c, :, piece(me)], send_y.at[1, c])
            )
        for copy in places:
            copy.start()
        for copy in places:
            copy.wait()

        def fetch(c):
            for copy in to_mate(c) + forward(c):
                copy.wait_recv()
            for copy in loads(c):
                copy.start()

        def compute(c):
            slot = lax.rem(c, 2)

            def block(t, carry):
                rows = pl.ds(pl.multiple_of(t * ROWS, ROWS), ROWS)
                pre = jnp.dot(x_ref[rows, :], up_slot[slot], preferred_element_type=jnp.float32)
                act = jax.nn.gelu(pre, approximate=True).astype(jnp.bfloat16)
                for n in range(0, total.shape[1], COLS):
                    total[rows, n : n + COLS] += jnp.dot(
                        act, down_slot[slot, :, n : n + COLS], preferred_element_type=jnp.float32
                    )

                @pl.when((t == 1) & (c + 1 < count))
                def _():
                    fetch(c + 1)

                return carry

            lax.fori_loop(0, tokens // ROWS, block, 0)

        def turn(c, carry):
            @pl.when(c < count)
            def _():
                @pl.when(c >= HEAD)
                def _():
                    for copy in down_link(c):
                        copy.wait_recv()

                for copy in to_across(c) + to_mate(c):
                    copy.start()

            @pl.when(c == 0)
            def _():
                total[...] = jnp.zeros_like(total)

            @pl.when((c >= 1) & (c <= count))
            def _():
                for copy in to_across(c - 1):
                    copy.wait_recv()
                for copy in forward(c - 1):
                    copy.start()

            @pl.when(c == 1)
            def _():
                fetch(0)
                x_copy.wait()

            @pl.when(c >= 2)
            def _():
                for copy in loads(c - 2):
                    copy.wait()
                compute(c - 2)

            return carry

        lax.fori_loop(0, count + 2, turn, 0)

        def out_copy(t):
            rows = pl.ds(pl.multiple_of(t * OUT_ROWS, OUT_ROWS), OUT_ROWS)
            slot = lax.rem(t, 2)
            return pltpu.make_async_copy(y_stage.at[slot], y_hbm.at[rows, :], y_sem.at[slot])

        def finish(t, carry):
            @pl.when(t >= 2)
            def _():
                out_copy(t - 2).wait()

            rows = pl.ds(pl.multiple_of(t * OUT_ROWS, OUT_ROWS), OUT_ROWS)
            y_stage[lax.rem(t, 2)] = (x_ref[rows, :].astype(jnp.float32) + total[rows, :]).astype(jnp.bfloat16)
            out_copy(t).start()
            return carry

        steps = tokens // OUT_ROWS
        lax.fori_loop(0, steps, finish, 0)

        def drain(c, carry):
            for copy in to_across(c) + to_mate(c) + forward(c):
                copy.wait_send()
            return carry

        lax.fori_loop(0, count, drain, 0)
        for t in (steps - 2, steps - 1):
            out_copy(t).wait()


def sweep(first, last, ins, outs, work):
    for i in (first, first + 1):
        for copy in ins(i):
            copy.start()

    def step(i, carry):
        @pl.when(i + 2 < last)
        def _():
            for copy in ins(i + 2):
                copy.start()

        for copy in ins(i):
            copy.wait()

        @pl.when(i >= first + DEPTH)
        def _():
            for copy in outs(i - DEPTH):
                copy.wait()

        work(lax.rem(i, DEPTH), i)
        for copy in outs(i):
            copy.start()
        return carry

    lax.fori_loop(first, last, step, 0)
    for i in range(last - DEPTH, last):
        for copy in outs(i):
            copy.wait()


def update_rows(first, last, tile, w, g, new, rate, w_buf, g_buf, n_buf, sems):
    def rows(i):
        return pl.ds(pl.multiple_of(i * tile, tile), tile)

    def ins(i):
        slot = lax.rem(i, DEPTH)
        return (
            pltpu.make_async_copy(w.at[rows(i), :], w_buf.at[slot], sems.at[0, slot]),
            pltpu.make_async_copy(g.at[rows(i), :], g_buf.at[slot], sems.at[1, slot]),
        )

    def outs(i):
        slot = lax.rem(i, DEPTH)
        return (pltpu.make_async_copy(n_buf.at[slot], new.at[rows(i), :], sems.at[2, slot]),)

    def work(slot, i):
        n_buf[slot] = w_buf[slot] - rate * g_buf[slot]

    sweep(first, last, ins, outs, work)


def early_kernel(up_w, up_g, rate_ref, up_new, down_new, w_buf, g_buf, n_buf, zero_down, sems, zero_sem):
    side = lax.axis_index("side")

    @pl.when(side == 0)
    def _():
        update_rows(0, EARLY, UP_TILE, up_w, up_g, up_new, rate_ref[0], w_buf, g_buf, n_buf, sems)

    @pl.when(side == 1)
    def _():
        n_buf[0] = jnp.zeros_like(n_buf[0])
        zero_down[...] = jnp.zeros_like(zero_down)
        copies = []
        for i in range(up_new.shape[0] // UP_TILE):
            copies.append(pltpu.make_async_copy(n_buf.at[0], up_new.at[pl.ds(i * UP_TILE, UP_TILE), :], zero_sem))
        for i in range(down_new.shape[0] // DOWN_TILE):
            copies.append(pltpu.make_async_copy(zero_down, down_new.at[pl.ds(i * DOWN_TILE, DOWN_TILE), :], zero_sem))
        for copy in copies:
            copy.start()
        for copy in copies:
            copy.wait()


def late_kernel(
    up_w, up_g, down_w, down_g, rate_ref, len_ref, y, up_in, down_in,
    up_new, down_new, out,
    w_buf, g_buf, n_buf, dw_buf, dg_buf, dn_buf, y_buf, o_buf, sems, d_sems, y_sems,
):
    side = lax.axis_index("side")
    steps = out.shape[0] // OUT_ROWS

    def rows(i):
        return pl.ds(pl.multiple_of(i * OUT_ROWS, OUT_ROWS), OUT_ROWS)

    @pl.when(side == 0)
    def _():
        rate = rate_ref[0]
        o_buf[0] = jnp.zeros_like(o_buf[0])
        zeros = [
            pltpu.make_async_copy(o_buf.at[0], out.at[pl.ds(i * OUT_ROWS, OUT_ROWS), :], y_sems.at[1, 0])
            for i in range(steps)
        ]
        for copy in zeros:
            copy.start()
        tiles = up_new.shape[0] // UP_TILE
        update_rows(EARLY, tiles, UP_TILE, up_w, up_g, up_new, rate, w_buf, g_buf, n_buf, sems)
        tiles = down_new.shape[0] // DOWN_TILE
        update_rows(0, tiles, DOWN_TILE, down_w, down_g, down_new, rate, dw_buf, dg_buf, dn_buf, d_sems)
        for copy in zeros:
            copy.wait()

    @pl.when(side == 1)
    def _():
        def ins(i):
            slot = lax.rem(i, DEPTH)
            return (pltpu.make_async_copy(y.at[rows(i), :], y_buf.at[slot], y_sems.at[0, slot]),)

        def outs(i):
            slot = lax.rem(i, DEPTH)
            return (pltpu.make_async_copy(o_buf.at[slot], out.at[rows(i), :], y_sems.at[1, slot]),)

        def work(slot, i):
            row = i * OUT_ROWS + lax.broadcasted_iota(jnp.int32, (OUT_ROWS, out.shape[1]), 0)
            tile = y_buf[slot]
            o_buf[slot] = jnp.where(row < len_ref[0], tile, jnp.zeros_like(tile))

        sweep(0, steps, ins, outs, work)


ANY = pl.BlockSpec(memory_space=pl.ANY)
SMEM = pl.BlockSpec(memory_space=pltpu.SMEM)
DMA = pltpu.SemaphoreType.DMA
F32 = jnp.float32
BF16 = jnp.bfloat16


def early(up_w, up_g, rate, down_shape):
    hidden = up_w.shape[1]
    band = pltpu.VMEM((DEPTH, UP_TILE, hidden), F32)
    return pl.pallas_call(
        early_kernel,
        out_shape=(jax.ShapeDtypeStruct(up_w.shape, F32), jax.ShapeDtypeStruct(down_shape, F32)),
        in_specs=[ANY, ANY, SMEM],
        out_specs=(ANY, ANY),
        scratch_shapes=[band] * 3 + [pltpu.VMEM((DOWN_TILE, down_shape[1]), F32), DMA((3, DEPTH)), DMA],
        compiler_params=pltpu.CompilerParams(vmem_limit_bytes=63 * 1024 * 1024),
        cost_estimate=pl.CostEstimate(flops=40_000_000, bytes_accessed=50_000_000, transcendentals=0),
    )(up_w, up_g, rate)


def late(up_w, up_g, down_w, down_g, rate, lens, y, up_new, down_new):
    hidden, width = down_w.shape
    up_band = pltpu.VMEM((DEPTH, UP_TILE, hidden), F32)
    down_band = pltpu.VMEM((DEPTH, DOWN_TILE, width), F32)
    row_band = pltpu.VMEM((DEPTH, OUT_ROWS, y.shape[1]), BF16)
    return pl.pallas_call(
        late_kernel,
        out_shape=(
            jax.ShapeDtypeStruct(up_w.shape, F32),
            jax.ShapeDtypeStruct(down_w.shape, F32),
            jax.ShapeDtypeStruct(y.shape, BF16),
        ),
        in_specs=[ANY] * 4 + [SMEM, SMEM] + [ANY] * 3,
        out_specs=(ANY,) * 3,
        scratch_shapes=[up_band] * 3 + [down_band] * 3 + [row_band] * 2
        + [DMA((3, DEPTH)), DMA((3, DEPTH)), DMA((2, DEPTH))],
        input_output_aliases={7: 0, 8: 1},
        compiler_params=pltpu.CompilerParams(vmem_limit_bytes=63 * 1024 * 1024),
        cost_estimate=pl.CostEstimate(flops=40_000_000, bytes_accessed=100_000_000, transcendentals=0),
    )(up_w, up_g, down_w, down_g, rate, lens, y, up_new, down_new)


def stream_mlp(up_w, up_g, down_w, down_g, rate, up_head, down_head, x, order):
    width, hidden = up_w.shape
    tokens, model = x.shape
    count = hidden // CHUNK
    return pl.pallas_call(
        stream_kernel,
        out_shape=(
            jax.ShapeDtypeStruct((tokens, model), BF16),
            jax.ShapeDtypeStruct((count, model, CHUNK), BF16),
            jax.ShapeDtypeStruct((count, CHUNK, model), BF16),
        ),
        in_specs=[ANY] * 4 + [SMEM] + [ANY] * 4,
        out_specs=(ANY,) * 3,
        scratch_shapes=[
            pltpu.VMEM((tokens, model), BF16),
            pltpu.VMEM((tokens, model), F32),
            pltpu.VMEM((2, model, CHUNK), BF16),
            pltpu.VMEM((2, CHUNK, model), BF16),
            pltpu.VMEM((width, HEAD * CHUNK), BF16),
            pltpu.VMEM((HEAD * CHUNK, width), BF16),
            pltpu.VMEM((2, OUT_ROWS, model), BF16),
        ]
        + [DMA((2, count))] * 8
        + [DMA((2, 2)), DMA((2, 4)), DMA((2,)), DMA, DMA((2,))],
        compiler_params=pltpu.CompilerParams(
            collective_id=0, has_side_effects=True, vmem_limit_bytes=63 * 1024 * 1024
        ),
        cost_estimate=pl.CostEstimate(
            flops=4 * tokens * model * hidden, bytes_accessed=8 * model * hidden, transcendentals=tokens * hidden
        ),
    )(up_w, up_g, down_w, down_g, rate, up_head, down_head, x, order)


def solution(mesh):
    up_spec = P("side", None, "rep", None)
    down_spec = P("side", None, None, "rep")
    act_spec = P("side", "rep", None)
    cross = [(r, r + mesh.shape["rep"]) for r in range(mesh.shape["rep"])]
    head = HEAD * CHUNK

    def device_step(w_up, w_down, g_up, g_down, learn_rate, prompts, prompt_lens):
        up_w, up_g, down_w, down_g = w_up[0, 0], g_up[0, 0], w_down[0, 0], g_down[0, 0]
        up_first = (up_w[:, :head] - learn_rate * up_g[:, :head]).astype(BF16)
        down_first = (down_w[:head, :] - learn_rate * down_g[:head, :]).astype(BF16)
        up_head = lax.ppermute(up_first, ("side", "rep"), cross)
        down_head = lax.ppermute(down_first, ("side", "rep"), cross)
        rate = learn_rate.reshape(1)
        up_part, down_part = early(up_w, up_g, rate, down_w.shape)
        y = stream_mlp(up_w, up_g, down_w, down_g, rate, up_head, down_head, prompts[0], down_part)[0]
        new_up, new_down, out = late(up_w, up_g, down_w, down_g, rate, prompt_lens, y, up_part, down_part)
        return new_up[None, None], new_down[None, None], out[None]

    return jax.shard_map(
        device_step,
        mesh=mesh,
        in_specs=(up_spec, down_spec, up_spec, down_spec, P(), act_spec, P("rep")),
        out_specs=(up_spec, down_spec, act_spec),
        check_vma=False,
    )
```

```python
import jax
import jax.numpy as jnp
from jax import lax
from jax.experimental import pallas as pl
from jax.experimental.pallas import tpu as pltpu
from jax.sharding import PartitionSpec as P

MESH = pl.DeviceIdType.MESH
CHUNK = 256
HEAD = 1
ROWS = 512
COLS = 768
OUT_ROWS = 256
UP_TILE = 32
DOWN_TILE = 512
EARLY = 14
OUT_SLOTS = ROWS // OUT_ROWS
LAG = 4
DEPTH = 3
STAGES = 4


def stream_kernel(
    up_w, up_g, down_w, down_g, rate_ref, up_head, down_head, x_hbm, order_ref,
    y_hbm, up_all, down_all,
    x_ref, total, up_slot, down_slot, up_bounce, down_bounce, y_stage,
    send_y, recv_y, send_x, recv_x, send_d, recv_d, send_f, recv_f,
    load_sem, fetch_sem, head_sem, x_sem, y_sem,
):
    side = lax.axis_index("side")
    me = lax.axis_index("rep")
    mate = me + 1 - 2 * lax.rem(me, 2)
    across = lax.rem(me + 2, 4)
    width = up_w.shape[0]
    count = up_w.shape[1] // CHUNK
    tokens = x_ref.shape[0]

    def meet():
        barrier = pltpu.get_barrier_semaphore()
        for peer in ((side, mate), (side, across), (1 - side, me)):
            pl.semaphore_signal(barrier, inc=1, device_id=peer, device_id_type=MESH)
        pl.semaphore_wait(barrier, 3)

    def wide(c):
        return pl.ds(pl.multiple_of(c * CHUNK, CHUNK), CHUNK)

    def piece(q):
        return pl.ds(pl.multiple_of(q * width, width), width)

    def remote(src, dst, send, recv, peer):
        return pltpu.make_async_remote_copy(
            src_ref=src, dst_ref=dst, send_sem=send, recv_sem=recv, device_id=peer, device_id_type=MESH
        )

    def down_link(c):
        stage = lax.rem(c, STAGES)
        up_part = up_slot.at[0, piece(stage), :]
        down_part = down_slot.at[0, :, piece(stage)]
        return (
            remote(up_part, up_all.at[c, piece(me), :], send_y.at[0, c], recv_y.at[0, c], (1, me)),
            remote(down_part, down_all.at[c, :, piece(me)], send_y.at[1, c], recv_y.at[1, c], (1, me)),
        )

    def relay(c, q, send, recv, peer):
        up_part = up_all.at[c, piece(q), :]
        down_part = down_all.at[c, :, piece(q)]
        return (
            remote(up_part, up_part, send.at[0, c], recv.at[0, c], (1, peer)),
            remote(down_part, down_part, send.at[1, c], recv.at[1, c], (1, peer)),
        )

    def to_across(c):
        return relay(c, me, send_x, recv_x, across)

    def to_mate(c):
        return relay(c, me, send_d, recv_d, mate)

    def forward(c):
        return relay(c, across, send_f, recv_f, mate)

    def loads(c):
        slot = lax.rem(c, 2)
        return (
            pltpu.make_async_copy(up_all.at[c], up_slot.at[slot], load_sem.at[0, slot]),
            pltpu.make_async_copy(down_all.at[c], down_slot.at[slot], load_sem.at[1, slot]),
        )

    @pl.when(side == 0)
    def _():
        rate = rate_ref[0]

        def up_view(slot, k):
            return total.at[pl.ds(0, width), pl.ds(pl.multiple_of((2 * slot + k) * CHUNK, CHUNK), CHUNK)]

        def down_view(slot, k):
            return total.at[pl.ds(pl.multiple_of(width + (2 * slot + k) * CHUNK, CHUNK), CHUNK), pl.ds(0, width)]

        def fetches(c):
            slot = lax.rem(c, 2)
            return (
                pltpu.make_async_copy(up_w.at[:, wide(c)], up_view(slot, 0), fetch_sem.at[slot, 0]),
                pltpu.make_async_copy(up_g.at[:, wide(c)], up_view(slot, 1), fetch_sem.at[slot, 1]),
                pltpu.make_async_copy(down_w.at[wide(c), :], down_view(slot, 0), fetch_sem.at[slot, 2]),
                pltpu.make_async_copy(down_g.at[wide(c), :], down_view(slot, 1), fetch_sem.at[slot, 3]),
            )

        for c in (HEAD, HEAD + 1):
            for copy in fetches(c):
                copy.start()
        meet()

        def send(c, carry):
            @pl.when(c < count)
            def _():
                for copy in fetches(c):
                    copy.wait()

            @pl.when(c > HEAD)
            def _():
                for copy in down_link(c - 1):
                    copy.start()

            @pl.when(c < count)
            def _():
                slot = lax.rem(c, 2)
                stage = lax.rem(c, STAGES)

                @pl.when(c >= HEAD + STAGES)
                def _():
                    for copy in down_link(c - STAGES):
                        copy.wait_send()

                up_slot[0, piece(stage), :] = (up_view(slot, 0)[...] - rate * up_view(slot, 1)[...]).astype(jnp.bfloat16)
                down_slot[0, :, piece(stage)] = (
                    down_view(slot, 0)[...] - rate * down_view(slot, 1)[...]
                ).astype(jnp.bfloat16)

                @pl.when(c + 2 < count)
                def _():
                    for copy in fetches(c + 2):
                        copy.start()

            return carry

        lax.fori_loop(HEAD, count + 1, send, 0)
        for c in range(count - STAGES, count):
            for copy in down_link(c):
                copy.wait_send()

    @pl.when(side == 1)
    def _():
        x_copy = pltpu.make_async_copy(x_hbm, x_ref, x_sem)
        heads = (
            pltpu.make_async_copy(up_head, up_bounce, head_sem.at[0]),
            pltpu.make_async_copy(down_head, down_bounce, head_sem.at[1]),
        )
        for copy in heads:
            copy.start()
        meet()
        for peer, send, recv in ((across, send_x, recv_x), (mate, send_d, recv_d)):
            remote(up_head, up_all.at[0, piece(me), :], send.at[0, 0], recv.at[0, 0], (1, peer)).start()
            remote(down_head, down_all.at[0, :, piece(me)], send.at[1, 0], recv.at[1, 0], (1, peer)).start()
        for copy in heads:
            copy.wait()
        places = (
            pltpu.make_async_copy(up_bounce, up_all.at[0, piece(me), :], head_sem.at[0]),
            pltpu.make_async_copy(down_bounce, down_all.at[0, :, piece(me)], head_sem.at[1]),
        )
        for copy in places:
            copy.start()
        x_copy.start()
        total[...] = jnp.zeros_like(total)
        for copy in places:
            copy.wait()
        x_copy.wait()

        def pass_on(c, half):
            down_link(c)[half].wait_recv()
            to_across(c)[half].start()
            to_mate(c)[half].start()

        def spread(c):
            for copy in to_across(c):
                copy.wait_recv()
            for copy in forward(c):
                copy.start()

        def settle(c):
            for copy in to_across(c) + to_mate(c) + forward(c):
                copy.wait_send()

        def out_copy(t):
            rows = pl.ds(pl.multiple_of(t * OUT_ROWS, OUT_ROWS), OUT_ROWS)
            slot = lax.rem(t, OUT_SLOTS)
            return pltpu.make_async_copy(y_stage.at[slot], y_hbm.at[rows, :], y_sem.at[slot])

        def block(c, t):
            slot = lax.rem(c, 2)
            rows = pl.ds(pl.multiple_of(t * ROWS, ROWS), ROWS)
            pre = jnp.dot(x_ref[rows, :], up_slot[slot], preferred_element_type=jnp.float32)
            act = jax.nn.gelu(pre, approximate=True).astype(jnp.bfloat16)
            for n in range(0, total.shape[1], COLS):
                total[rows, n : n + COLS] += jnp.dot(
                    act, down_slot[slot, :, n : n + COLS], preferred_element_type=jnp.float32
                )

            @pl.when(c == count - 1)
            def _():
                for j in range(OUT_SLOTS):
                    k = t * OUT_SLOTS + j

                    @pl.when(t > 0)
                    def _():
                        out_copy(k - OUT_SLOTS).wait()

                    part = pl.ds(pl.multiple_of(k * OUT_ROWS, OUT_ROWS), OUT_ROWS)
                    y_stage[j] = (x_ref[part, :].astype(jnp.float32) + total[part, :]).astype(jnp.bfloat16)
                    out_copy(k).start()

        last = tokens // ROWS - 1
        pass_on(1, 0)
        spread(0)

        def turn(c, carry):
            @pl.when(c < count)
            def _():
                pass_on(c, 1)

            @pl.when(c <= count)
            def _():
                for copy in to_mate(c - 1) + forward(c - 1):
                    copy.wait_recv()
                for copy in loads(c - 1):
                    copy.start()

            @pl.when(c >= 2)
            def _():
                block(c - 2, last)

            @pl.when(c <= count)
            def _():
                for copy in loads(c - 1):
                    copy.wait()

                def part(t, carry):
                    block(c - 1, t)
                    return carry

                lax.fori_loop(0, last, part, 0)

            @pl.when(c + 1 < count)
            def _():
                pass_on(c + 1, 0)

            @pl.when(c < count)
            def _():
                spread(c)

            @pl.when(c >= LAG)
            def _():
                settle(c - LAG)

            return carry

        lax.fori_loop(1, count + 2, turn, 0)
        for c in range(count + 2 - LAG, count):
            settle(c)
        for k in range((last + 1) * OUT_SLOTS - OUT_SLOTS, (last + 1) * OUT_SLOTS):
            out_copy(k).wait()


def sweep(first, last, ins, outs, work):
    for i in (first, first + 1):
        for copy in ins(i):
            copy.start()

    def step(i, carry):
        @pl.when(i + 2 < last)
        def _():
            for copy in ins(i + 2):
                copy.start()

        for copy in ins(i):
            copy.wait()

        @pl.when(i >= first + DEPTH)
        def _():
            for copy in outs(i - DEPTH):
                copy.wait()

        work(lax.rem(i, DEPTH), i)
        for copy in outs(i):
            copy.start()
        return carry

    lax.fori_loop(first, last, step, 0)
    for i in range(last - DEPTH, last):
        for copy in outs(i):
            copy.wait()


def update_rows(first, last, tile, w, g, new, rate, w_buf, g_buf, n_buf, sems):
    def rows(i):
        return pl.ds(pl.multiple_of(i * tile, tile), tile)

    def ins(i):
        slot = lax.rem(i, DEPTH)
        return (
            pltpu.make_async_copy(w.at[rows(i), :], w_buf.at[slot], sems.at[0, slot]),
            pltpu.make_async_copy(g.at[rows(i), :], g_buf.at[slot], sems.at[1, slot]),
        )

    def outs(i):
        slot = lax.rem(i, DEPTH)
        return (pltpu.make_async_copy(n_buf.at[slot], new.at[rows(i), :], sems.at[2, slot]),)

    def work(slot, i):
        n_buf[slot] = w_buf[slot] - rate * g_buf[slot]

    sweep(first, last, ins, outs, work)


def early_kernel(up_w, up_g, rate_ref, up_new, down_new, w_buf, g_buf, n_buf, zero_down, sems, zero_sem):
    side = lax.axis_index("side")

    @pl.when(side == 0)
    def _():
        update_rows(0, EARLY, UP_TILE, up_w, up_g, up_new, rate_ref[0], w_buf, g_buf, n_buf, sems)

    @pl.when(side == 1)
    def _():
        n_buf[0] = jnp.zeros_like(n_buf[0])
        zero_down[...] = jnp.zeros_like(zero_down)
        copies = []
        for i in range(up_new.shape[0] // UP_TILE):
            copies.append(pltpu.make_async_copy(n_buf.at[0], up_new.at[pl.ds(i * UP_TILE, UP_TILE), :], zero_sem))
        for i in range(down_new.shape[0] // DOWN_TILE):
            copies.append(pltpu.make_async_copy(zero_down, down_new.at[pl.ds(i * DOWN_TILE, DOWN_TILE), :], zero_sem))
        for copy in copies:
            copy.start()
        for copy in copies:
            copy.wait()


def late_kernel(
    up_w, up_g, down_w, down_g, rate_ref, len_ref, y, up_in, down_in,
    up_new, down_new, out,
    w_buf, g_buf, n_buf, dw_buf, dg_buf, dn_buf, y_buf, o_buf, sems, d_sems, y_sems,
):
    side = lax.axis_index("side")
    steps = out.shape[0] // OUT_ROWS

    def rows(i):
        return pl.ds(pl.multiple_of(i * OUT_ROWS, OUT_ROWS), OUT_ROWS)

    @pl.when(side == 0)
    def _():
        rate = rate_ref[0]
        o_buf[0] = jnp.zeros_like(o_buf[0])
        zeros = [
            pltpu.make_async_copy(o_buf.at[0], out.at[pl.ds(i * OUT_ROWS, OUT_ROWS), :], y_sems.at[1, 0])
            for i in range(steps)
        ]
        for copy in zeros:
            copy.start()
        tiles = up_new.shape[0] // UP_TILE
        update_rows(EARLY, tiles, UP_TILE, up_w, up_g, up_new, rate, w_buf, g_buf, n_buf, sems)
        tiles = down_new.shape[0] // DOWN_TILE
        update_rows(0, tiles, DOWN_TILE, down_w, down_g, down_new, rate, dw_buf, dg_buf, dn_buf, d_sems)
        for copy in zeros:
            copy.wait()

    @pl.when(side == 1)
    def _():
        def ins(i):
            slot = lax.rem(i, DEPTH)
            return (pltpu.make_async_copy(y.at[rows(i), :], y_buf.at[slot], y_sems.at[0, slot]),)

        def outs(i):
            slot = lax.rem(i, DEPTH)
            return (pltpu.make_async_copy(o_buf.at[slot], out.at[rows(i), :], y_sems.at[1, slot]),)

        def work(slot, i):
            row = i * OUT_ROWS + lax.broadcasted_iota(jnp.int32, (OUT_ROWS, out.shape[1]), 0)
            tile = y_buf[slot]
            o_buf[slot] = jnp.where(row < len_ref[0], tile, jnp.zeros_like(tile))

        sweep(0, steps, ins, outs, work)


ANY = pl.BlockSpec(memory_space=pl.ANY)
SMEM = pl.BlockSpec(memory_space=pltpu.SMEM)
DMA = pltpu.SemaphoreType.DMA
F32 = jnp.float32
BF16 = jnp.bfloat16


def early(up_w, up_g, rate, down_shape):
    hidden = up_w.shape[1]
    band = pltpu.VMEM((DEPTH, UP_TILE, hidden), F32)
    return pl.pallas_call(
        early_kernel,
        out_shape=(jax.ShapeDtypeStruct(up_w.shape, F32), jax.ShapeDtypeStruct(down_shape, F32)),
        in_specs=[ANY, ANY, SMEM],
        out_specs=(ANY, ANY),
        scratch_shapes=[band] * 3 + [pltpu.VMEM((DOWN_TILE, down_shape[1]), F32), DMA((3, DEPTH)), DMA],
        compiler_params=pltpu.CompilerParams(vmem_limit_bytes=63 * 1024 * 1024),
        cost_estimate=pl.CostEstimate(flops=40_000_000, bytes_accessed=50_000_000, transcendentals=0),
    )(up_w, up_g, rate)


def late(up_w, up_g, down_w, down_g, rate, lens, y, up_new, down_new):
    hidden, width = down_w.shape
    up_band = pltpu.VMEM((DEPTH, UP_TILE, hidden), F32)
    down_band = pltpu.VMEM((DEPTH, DOWN_TILE, width), F32)
    row_band = pltpu.VMEM((DEPTH, OUT_ROWS, y.shape[1]), BF16)
    return pl.pallas_call(
        late_kernel,
        out_shape=(
            jax.ShapeDtypeStruct(up_w.shape, F32),
            jax.ShapeDtypeStruct(down_w.shape, F32),
            jax.ShapeDtypeStruct(y.shape, BF16),
        ),
        in_specs=[ANY] * 4 + [SMEM, SMEM] + [ANY] * 3,
        out_specs=(ANY,) * 3,
        scratch_shapes=[up_band] * 3 + [down_band] * 3 + [row_band] * 2
        + [DMA((3, DEPTH)), DMA((3, DEPTH)), DMA((2, DEPTH))],
        input_output_aliases={7: 0, 8: 1},
        compiler_params=pltpu.CompilerParams(vmem_limit_bytes=63 * 1024 * 1024),
        cost_estimate=pl.CostEstimate(flops=40_000_000, bytes_accessed=100_000_000, transcendentals=0),
    )(up_w, up_g, down_w, down_g, rate, lens, y, up_new, down_new)


def stream_mlp(up_w, up_g, down_w, down_g, rate, up_head, down_head, x, order):
    width, hidden = up_w.shape
    tokens, model = x.shape
    count = hidden // CHUNK
    return pl.pallas_call(
        stream_kernel,
        out_shape=(
            jax.ShapeDtypeStruct((tokens, model), BF16),
            jax.ShapeDtypeStruct((count, model, CHUNK), BF16),
            jax.ShapeDtypeStruct((count, CHUNK, model), BF16),
        ),
        in_specs=[ANY] * 4 + [SMEM] + [ANY] * 4,
        out_specs=(ANY,) * 3,
        scratch_shapes=[
            pltpu.VMEM((tokens, model), BF16),
            pltpu.VMEM((tokens, model), F32),
            pltpu.VMEM((2, model, CHUNK), BF16),
            pltpu.VMEM((2, CHUNK, model), BF16),
            pltpu.VMEM((width, HEAD * CHUNK), BF16),
            pltpu.VMEM((HEAD * CHUNK, width), BF16),
            pltpu.VMEM((OUT_SLOTS, OUT_ROWS, model), BF16),
        ]
        + [DMA((2, count))] * 8
        + [DMA((2, 2)), DMA((2, 4)), DMA((2,)), DMA, DMA((2,))],
        compiler_params=pltpu.CompilerParams(
            collective_id=0, has_side_effects=True, vmem_limit_bytes=63 * 1024 * 1024
        ),
        cost_estimate=pl.CostEstimate(
            flops=4 * tokens * model * hidden, bytes_accessed=8 * model * hidden, transcendentals=tokens * hidden
        ),
    )(up_w, up_g, down_w, down_g, rate, up_head, down_head, x, order)


def solution(mesh):
    up_spec = P("side", None, "rep", None)
    down_spec = P("side", None, None, "rep")
    act_spec = P("side", "rep", None)
    cross = [(r, r + mesh.shape["rep"]) for r in range(mesh.shape["rep"])]
    head = HEAD * CHUNK

    def device_step(w_up, w_down, g_up, g_down, learn_rate, prompts, prompt_lens):
        up_w, up_g, down_w, down_g = w_up[0, 0], g_up[0, 0], w_down[0, 0], g_down[0, 0]
        up_first = (up_w[:, :head] - learn_rate * up_g[:, :head]).astype(BF16)
        down_first = (down_w[:head, :] - learn_rate * down_g[:head, :]).astype(BF16)
        up_head = lax.ppermute(up_first, ("side", "rep"), cross)
        down_head = lax.ppermute(down_first, ("side", "rep"), cross)
        rate = learn_rate.reshape(1)
        up_part, down_part = early(up_w, up_g, rate, down_w.shape)
        y = stream_mlp(up_w, up_g, down_w, down_g, rate, up_head, down_head, prompts[0], down_part)[0]
        new_up, new_down, out = late(up_w, up_g, down_w, down_g, rate, prompt_lens, y, up_part, down_part)
        return new_up[None, None], new_down[None, None], out[None]

    return jax.shard_map(
        device_step,
        mesh=mesh,
        in_specs=(up_spec, down_spec, up_spec, down_spec, P(), act_spec, P("rep")),
        out_specs=(up_spec, down_spec, act_spec),
        check_vma=False,
    )
```

```python
import jax
import jax.numpy as jnp
from jax import lax
from jax.experimental import pallas as pl
from jax.experimental.pallas import tpu as pltpu
from jax.sharding import PartitionSpec as P

MESH = pl.DeviceIdType.MESH
CHUNK = 256
HEAD = 1
ROWS = 512
COLS = 768
OUT_ROWS = 256
UP_TILE = 32
DOWN_TILE = 512
EARLY = 12
OUT_SLOTS = ROWS // OUT_ROWS
LAG = 4
DEPTH = 3
STAGES = 4


def stream_kernel(
    up_w, up_g, down_w, down_g, rate_ref, up_head, down_head, x_hbm, order_ref,
    y_hbm, up_all, down_all,
    x_ref, total, up_slot, down_slot, up_bounce, down_bounce, y_stage,
    send_y, recv_y, send_x, recv_x, send_d, recv_d, send_f, recv_f,
    load_sem, fetch_sem, head_sem, x_sem, y_sem,
):
    side = lax.axis_index("side")
    me = lax.axis_index("rep")
    mate = me + 1 - 2 * lax.rem(me, 2)
    across = lax.rem(me + 2, 4)
    width = up_w.shape[0]
    count = up_w.shape[1] // CHUNK
    tokens = x_ref.shape[0]

    def meet():
        barrier = pltpu.get_barrier_semaphore()
        for peer in ((side, mate), (side, across), (1 - side, me)):
            pl.semaphore_signal(barrier, inc=1, device_id=peer, device_id_type=MESH)
        pl.semaphore_wait(barrier, 3)

    def wide(c):
        return pl.ds(pl.multiple_of(c * CHUNK, CHUNK), CHUNK)

    def piece(q):
        return pl.ds(pl.multiple_of(q * width, width), width)

    def remote(src, dst, send, recv, peer):
        return pltpu.make_async_remote_copy(
            src_ref=src, dst_ref=dst, send_sem=send, recv_sem=recv, device_id=peer, device_id_type=MESH
        )

    def down_link(c):
        stage = lax.rem(c, STAGES)
        up_part = up_slot.at[0, piece(stage), :]
        down_part = down_slot.at[0, :, piece(stage)]
        return (
            remote(up_part, up_all.at[c, piece(me), :], send_y.at[0, c], recv_y.at[0, c], (1, me)),
            remote(down_part, down_all.at[c, :, piece(me)], send_y.at[1, c], recv_y.at[1, c], (1, me)),
        )

    def relay(c, q, send, recv, peer):
        up_part = up_all.at[c, piece(q), :]
        down_part = down_all.at[c, :, piece(q)]
        return (
            remote(up_part, up_part, send.at[0, c], recv.at[0, c], (1, peer)),
            remote(down_part, down_part, send.at[1, c], recv.at[1, c], (1, peer)),
        )

    def to_across(c):
        return relay(c, me, send_x, recv_x, across)

    def to_mate(c):
        return relay(c, me, send_d, recv_d, mate)

    def forward(c):
        return relay(c, across, send_f, recv_f, mate)

    def loads(c):
        slot = lax.rem(c, 2)
        return (
            pltpu.make_async_copy(up_all.at[c], up_slot.at[slot], load_sem.at[0, slot]),
            pltpu.make_async_copy(down_all.at[c], down_slot.at[slot], load_sem.at[1, slot]),
        )

    @pl.when(side == 0)
    def _():
        rate = rate_ref[0]

        def up_view(slot, k):
            return total.at[pl.ds(0, width), pl.ds(pl.multiple_of((2 * slot + k) * CHUNK, CHUNK), CHUNK)]

        def down_view(slot, k):
            return total.at[pl.ds(pl.multiple_of(width + (2 * slot + k) * CHUNK, CHUNK), CHUNK), pl.ds(0, width)]

        def fetches(c):
            slot = lax.rem(c, 2)
            return (
                pltpu.make_async_copy(up_w.at[:, wide(c)], up_view(slot, 0), fetch_sem.at[slot, 0]),
                pltpu.make_async_copy(up_g.at[:, wide(c)], up_view(slot, 1), fetch_sem.at[slot, 1]),
                pltpu.make_async_copy(down_w.at[wide(c), :], down_view(slot, 0), fetch_sem.at[slot, 2]),
                pltpu.make_async_copy(down_g.at[wide(c), :], down_view(slot, 1), fetch_sem.at[slot, 3]),
            )

        for c in (HEAD, HEAD + 1):
            for copy in fetches(c):
                copy.start()
        meet()

        def send(c, carry):
            @pl.when(c < count)
            def _():
                for copy in fetches(c):
                    copy.wait()

            @pl.when(c > HEAD)
            def _():
                for copy in down_link(c - 1):
                    copy.start()

            @pl.when(c < count)
            def _():
                slot = lax.rem(c, 2)
                stage = lax.rem(c, STAGES)

                @pl.when(c >= HEAD + STAGES)
                def _():
                    for copy in down_link(c - STAGES):
                        copy.wait_send()

                up_slot[0, piece(stage), :] = (up_view(slot, 0)[...] - rate * up_view(slot, 1)[...]).astype(jnp.bfloat16)
                down_slot[0, :, piece(stage)] = (
                    down_view(slot, 0)[...] - rate * down_view(slot, 1)[...]
                ).astype(jnp.bfloat16)

                @pl.when(c + 2 < count)
                def _():
                    for copy in fetches(c + 2):
                        copy.start()

            return carry

        lax.fori_loop(HEAD, count + 1, send, 0)
        for c in range(count - STAGES, count):
            for copy in down_link(c):
                copy.wait_send()

    @pl.when(side == 1)
    def _():
        x_copy = pltpu.make_async_copy(x_hbm, x_ref, x_sem)
        heads = (
            pltpu.make_async_copy(up_head, up_bounce, head_sem.at[0]),
            pltpu.make_async_copy(down_head, down_bounce, head_sem.at[1]),
        )
        for copy in heads:
            copy.start()
        meet()
        for peer, send, recv in ((across, send_x, recv_x), (mate, send_d, recv_d)):
            remote(up_head, up_all.at[0, piece(me), :], send.at[0, 0], recv.at[0, 0], (1, peer)).start()
            remote(down_head, down_all.at[0, :, piece(me)], send.at[1, 0], recv.at[1, 0], (1, peer)).start()
        for copy in heads:
            copy.wait()
        places = (
            pltpu.make_async_copy(up_bounce, up_all.at[0, piece(me), :], head_sem.at[0]),
            pltpu.make_async_copy(down_bounce, down_all.at[0, :, piece(me)], head_sem.at[1]),
        )
        for copy in places:
            copy.start()
        x_copy.start()
        total[...] = jnp.zeros_like(total)
        for copy in places:
            copy.wait()
        x_copy.wait()

        def pass_on(c, half):
            down_link(c)[half].wait_recv()
            to_across(c)[half].start()
            to_mate(c)[half].start()

        def spread(c):
            for copy in to_across(c):
                copy.wait_recv()
            for copy in forward(c):
                copy.start()

        def settle(c):
            for copy in to_across(c) + to_mate(c) + forward(c):
                copy.wait_send()

        def out_copy(t):
            rows = pl.ds(pl.multiple_of(t * OUT_ROWS, OUT_ROWS), OUT_ROWS)
            slot = lax.rem(t, OUT_SLOTS)
            return pltpu.make_async_copy(y_stage.at[slot], y_hbm.at[rows, :], y_sem.at[slot])

        def block(c, t):
            slot = lax.rem(c, 2)
            rows = pl.ds(pl.multiple_of(t * ROWS, ROWS), ROWS)
            pre = jnp.dot(x_ref[rows, :], up_slot[slot], preferred_element_type=jnp.float32)
            act = jax.nn.gelu(pre, approximate=True).astype(jnp.bfloat16)
            for n in range(0, total.shape[1], COLS):
                total[rows, n : n + COLS] += jnp.dot(
                    act, down_slot[slot, :, n : n + COLS], preferred_element_type=jnp.float32
                )

            @pl.when(c == count - 1)
            def _():
                for j in range(OUT_SLOTS):
                    k = t * OUT_SLOTS + j

                    @pl.when(t > 0)
                    def _():
                        out_copy(k - OUT_SLOTS).wait()

                    part = pl.ds(pl.multiple_of(k * OUT_ROWS, OUT_ROWS), OUT_ROWS)
                    y_stage[j] = (x_ref[part, :].astype(jnp.float32) + total[part, :]).astype(jnp.bfloat16)
                    out_copy(k).start()

        blocks = tokens // ROWS
        half = blocks // 2
        assert blocks == 4
        pass_on(1, 0)
        spread(0)

        def turn(c, carry):
            @pl.when(c < count)
            def _():
                pass_on(c, 1)

            @pl.when(c >= 2)
            def _():
                block(c - 2, half)

            @pl.when(c <= count)
            def _():
                for copy in to_mate(c - 1) + forward(c - 1):
                    copy.wait_recv()
                for copy in loads(c - 1):
                    copy.start()

            @pl.when(c >= 2)
            def _():
                block(c - 2, half + 1)

            @pl.when(c <= count)
            def _():
                for copy in loads(c - 1):
                    copy.wait()

                def part(t, carry):
                    block(c - 1, t)
                    return carry

                lax.fori_loop(0, half, part, 0)

            @pl.when(c + 1 < count)
            def _():
                pass_on(c + 1, 0)

            @pl.when(c < count)
            def _():
                spread(c)

            @pl.when(c >= LAG)
            def _():
                settle(c - LAG)

            return carry

        lax.fori_loop(1, count + 2, turn, 0)
        for c in range(count + 2 - LAG, count):
            settle(c)
        for k in range((blocks - 1) * OUT_SLOTS, blocks * OUT_SLOTS):
            out_copy(k).wait()


def sweep(first, last, ins, outs, work):
    for i in (first, first + 1):
        for copy in ins(i):
            copy.start()

    def step(i, carry):
        @pl.when(i + 2 < last)
        def _():
            for copy in ins(i + 2):
                copy.start()

        for copy in ins(i):
            copy.wait()

        @pl.when(i >= first + DEPTH)
        def _():
            for copy in outs(i - DEPTH):
                copy.wait()

        work(lax.rem(i, DEPTH), i)
        for copy in outs(i):
            copy.start()
        return carry

    lax.fori_loop(first, last, step, 0)
    for i in range(last - DEPTH, last):
        for copy in outs(i):
            copy.wait()


def update_rows(first, last, tile, w, g, new, rate, w_buf, g_buf, n_buf, sems):
    def rows(i):
        return pl.ds(pl.multiple_of(i * tile, tile), tile)

    def ins(i):
        slot = lax.rem(i, DEPTH)
        return (
            pltpu.make_async_copy(w.at[rows(i), :], w_buf.at[slot], sems.at[0, slot]),
            pltpu.make_async_copy(g.at[rows(i), :], g_buf.at[slot], sems.at[1, slot]),
        )

    def outs(i):
        slot = lax.rem(i, DEPTH)
        return (pltpu.make_async_copy(n_buf.at[slot], new.at[rows(i), :], sems.at[2, slot]),)

    def work(slot, i):
        n_buf[slot] = w_buf[slot] - rate * g_buf[slot]

    sweep(first, last, ins, outs, work)


def early_kernel(up_w, up_g, rate_ref, up_new, down_new, w_buf, g_buf, n_buf, zero_down, sems, zero_sem):
    side = lax.axis_index("side")

    @pl.when(side == 0)
    def _():
        update_rows(0, EARLY, UP_TILE, up_w, up_g, up_new, rate_ref[0], w_buf, g_buf, n_buf, sems)

    @pl.when(side == 1)
    def _():
        n_buf[0] = jnp.zeros_like(n_buf[0])
        zero_down[...] = jnp.zeros_like(zero_down)
        copies = []
        for i in range(up_new.shape[0] // UP_TILE):
            copies.append(pltpu.make_async_copy(n_buf.at[0], up_new.at[pl.ds(i * UP_TILE, UP_TILE), :], zero_sem))
        for i in range(down_new.shape[0] // DOWN_TILE):
            copies.append(pltpu.make_async_copy(zero_down, down_new.at[pl.ds(i * DOWN_TILE, DOWN_TILE), :], zero_sem))
        for copy in copies:
            copy.start()
        for copy in copies:
            copy.wait()


def late_kernel(
    up_w, up_g, down_w, down_g, rate_ref, len_ref, y, up_in, down_in,
    up_new, down_new, out,
    w_buf, g_buf, n_buf, dw_buf, dg_buf, dn_buf, y_buf, o_buf, sems, d_sems, y_sems,
):
    side = lax.axis_index("side")
    steps = out.shape[0] // OUT_ROWS

    def rows(i):
        return pl.ds(pl.multiple_of(i * OUT_ROWS, OUT_ROWS), OUT_ROWS)

    @pl.when(side == 0)
    def _():
        rate = rate_ref[0]
        o_buf[0] = jnp.zeros_like(o_buf[0])
        zeros = [
            pltpu.make_async_copy(o_buf.at[0], out.at[pl.ds(i * OUT_ROWS, OUT_ROWS), :], y_sems.at[1, 0])
            for i in range(steps)
        ]
        for copy in zeros:
            copy.start()
        tiles = up_new.shape[0] // UP_TILE
        update_rows(EARLY, tiles, UP_TILE, up_w, up_g, up_new, rate, w_buf, g_buf, n_buf, sems)
        tiles = down_new.shape[0] // DOWN_TILE
        update_rows(0, tiles, DOWN_TILE, down_w, down_g, down_new, rate, dw_buf, dg_buf, dn_buf, d_sems)
        for copy in zeros:
            copy.wait()

    @pl.when(side == 1)
    def _():
        def ins(i):
            slot = lax.rem(i, DEPTH)
            return (pltpu.make_async_copy(y.at[rows(i), :], y_buf.at[slot], y_sems.at[0, slot]),)

        def outs(i):
            slot = lax.rem(i, DEPTH)
            return (pltpu.make_async_copy(o_buf.at[slot], out.at[rows(i), :], y_sems.at[1, slot]),)

        def work(slot, i):
            row = i * OUT_ROWS + lax.broadcasted_iota(jnp.int32, (OUT_ROWS, out.shape[1]), 0)
            tile = y_buf[slot]
            o_buf[slot] = jnp.where(row < len_ref[0], tile, jnp.zeros_like(tile))

        sweep(0, steps, ins, outs, work)


ANY = pl.BlockSpec(memory_space=pl.ANY)
SMEM = pl.BlockSpec(memory_space=pltpu.SMEM)
DMA = pltpu.SemaphoreType.DMA
F32 = jnp.float32
BF16 = jnp.bfloat16


def early(up_w, up_g, rate, down_shape):
    hidden = up_w.shape[1]
    band = pltpu.VMEM((DEPTH, UP_TILE, hidden), F32)
    return pl.pallas_call(
        early_kernel,
        out_shape=(jax.ShapeDtypeStruct(up_w.shape, F32), jax.ShapeDtypeStruct(down_shape, F32)),
        in_specs=[ANY, ANY, SMEM],
        out_specs=(ANY, ANY),
        scratch_shapes=[band] * 3 + [pltpu.VMEM((DOWN_TILE, down_shape[1]), F32), DMA((3, DEPTH)), DMA],
        compiler_params=pltpu.CompilerParams(vmem_limit_bytes=63 * 1024 * 1024),
        cost_estimate=pl.CostEstimate(flops=40_000_000, bytes_accessed=50_000_000, transcendentals=0),
    )(up_w, up_g, rate)


def late(up_w, up_g, down_w, down_g, rate, lens, y, up_new, down_new):
    hidden, width = down_w.shape
    up_band = pltpu.VMEM((DEPTH, UP_TILE, hidden), F32)
    down_band = pltpu.VMEM((DEPTH, DOWN_TILE, width), F32)
    row_band = pltpu.VMEM((DEPTH, OUT_ROWS, y.shape[1]), BF16)
    return pl.pallas_call(
        late_kernel,
        out_shape=(
            jax.ShapeDtypeStruct(up_w.shape, F32),
            jax.ShapeDtypeStruct(down_w.shape, F32),
            jax.ShapeDtypeStruct(y.shape, BF16),
        ),
        in_specs=[ANY] * 4 + [SMEM, SMEM] + [ANY] * 3,
        out_specs=(ANY,) * 3,
        scratch_shapes=[up_band] * 3 + [down_band] * 3 + [row_band] * 2
        + [DMA((3, DEPTH)), DMA((3, DEPTH)), DMA((2, DEPTH))],
        input_output_aliases={7: 0, 8: 1},
        compiler_params=pltpu.CompilerParams(vmem_limit_bytes=63 * 1024 * 1024),
        cost_estimate=pl.CostEstimate(flops=40_000_000, bytes_accessed=100_000_000, transcendentals=0),
    )(up_w, up_g, down_w, down_g, rate, lens, y, up_new, down_new)


def stream_mlp(up_w, up_g, down_w, down_g, rate, up_head, down_head, x, order):
    width, hidden = up_w.shape
    tokens, model = x.shape
    count = hidden // CHUNK
    return pl.pallas_call(
        stream_kernel,
        out_shape=(
            jax.ShapeDtypeStruct((tokens, model), BF16),
            jax.ShapeDtypeStruct((count, model, CHUNK), BF16),
            jax.ShapeDtypeStruct((count, CHUNK, model), BF16),
        ),
        in_specs=[ANY] * 4 + [SMEM] + [ANY] * 4,
        out_specs=(ANY,) * 3,
        scratch_shapes=[
            pltpu.VMEM((tokens, model), BF16),
            pltpu.VMEM((tokens, model), F32),
            pltpu.VMEM((2, model, CHUNK), BF16),
            pltpu.VMEM((2, CHUNK, model), BF16),
            pltpu.VMEM((width, HEAD * CHUNK), BF16),
            pltpu.VMEM((HEAD * CHUNK, width), BF16),
            pltpu.VMEM((OUT_SLOTS, OUT_ROWS, model), BF16),
        ]
        + [DMA((2, count))] * 8
        + [DMA((2, 2)), DMA((2, 4)), DMA((2,)), DMA, DMA((2,))],
        compiler_params=pltpu.CompilerParams(
            collective_id=0, has_side_effects=True, vmem_limit_bytes=63 * 1024 * 1024
        ),
        cost_estimate=pl.CostEstimate(
            flops=4 * tokens * model * hidden, bytes_accessed=8 * model * hidden, transcendentals=tokens * hidden
        ),
    )(up_w, up_g, down_w, down_g, rate, up_head, down_head, x, order)


def solution(mesh):
    up_spec = P("side", None, "rep", None)
    down_spec = P("side", None, None, "rep")
    act_spec = P("side", "rep", None)
    cross = [(r, r + mesh.shape["rep"]) for r in range(mesh.shape["rep"])]
    head = HEAD * CHUNK

    def device_step(w_up, w_down, g_up, g_down, learn_rate, prompts, prompt_lens):
        up_w, up_g, down_w, down_g = w_up[0, 0], g_up[0, 0], w_down[0, 0], g_down[0, 0]
        up_first = (up_w[:, :head] - learn_rate * up_g[:, :head]).astype(BF16)
        down_first = (down_w[:head, :] - learn_rate * down_g[:head, :]).astype(BF16)
        up_head = lax.ppermute(up_first, ("side", "rep"), cross)
        down_head = lax.ppermute(down_first, ("side", "rep"), cross)
        rate = learn_rate.reshape(1)
        up_part, down_part = early(up_w, up_g, rate, down_w.shape)
        y = stream_mlp(up_w, up_g, down_w, down_g, rate, up_head, down_head, prompts[0], down_part)[0]
        new_up, new_down, out = late(up_w, up_g, down_w, down_g, rate, prompt_lens, y, up_part, down_part)
        return new_up[None, None], new_down[None, None], out[None]

    return jax.shard_map(
        device_step,
        mesh=mesh,
        in_specs=(up_spec, down_spec, up_spec, down_spec, P(), act_spec, P("rep")),
        out_specs=(up_spec, down_spec, act_spec),
        check_vma=False,
    )
```
